32 devices in a mesh: dp: 4 (over x, core), expert: 8 (over z, y).
Axes of the slice: x: 2, y: 2, z: 4, core: 2. Of those that a mesh axis runs over, the one named last changes fastest.
Arguments:
- tokens: bfloat16 [4096, 2048], P(('dp', 'expert')), may hold values from -6 to 6
- norm_gain: bfloat16 [2048], replicated, may hold values from 0.099609375 to 1.8984375
- router_weight: bfloat16 [2048, 8], replicated, may hold values from -0.1875 to 0.1875
- w_gate: bfloat16 [8, 2048, 5120], P('expert', None, 'dp'), may hold values from -0.125 to 0.125
- w_up: bfloat16 [8, 2048, 5120], P('expert', None, 'dp'), may hold values from -0.125 to 0.125
- w_down: bfloat16 [8, 5120, 2048], P('expert', 'dp'), may hold values from -0.078125 to 0.078125
- selected: int32 [8, 896], replicated, may hold values from 0 to 4095, as said below
Outputs:
- combined: bfloat16 [4096, 2048], P(('dp', 'expert'))
The draws below stay inside these ranges and needn't reach their ends.
Inputs may be any that keep to these rules, and one draw needn't show every extreme that they name: `selected`: each row holds 896 distinct token indices in ascending order. Of one row's indices at most 64 fall among one device's 128 tokens and at most 336 among the tokens of one index of dp; every row reaches both bounds.
All inputs are finite; a program needn't handle non-finite values.
Results may differ from the reference program's by a relative error of at most 0.0072.
Values may be sent and summed in bfloat16 or wider, within the bound.
A program may use at most 128 MiB of HBM per device.

```python
import jax
import jax.numpy as jnp
from jax import lax

D = 2048
FF = 5120
TOK_DEV = 128
EXPERTS = 8
TOKENS = 4096
CAP = 896
PEAK = 64
RMOST = 336
N_DP = 4
N_EXPERT = 8


def choose_tokens(key):
    keys = jax.random.split(key, 7)
    row_cells = N_DP * RMOST
    row_score = jax.random.randint(keys[0], (N_DP, RMOST), 0, 1024) + 1024 * jax.random.randint(keys[1], (N_DP, 1), 0, 16)
    forced_row = jax.random.randint(keys[2], (), 0, N_DP)
    row_score = row_score + jnp.where(jnp.arange(N_DP) == forced_row, 32768, 0)[:, None]
    row_distinct = row_score.reshape(-1) * row_cells + jnp.arange(row_cells)
    row_order = jnp.argsort(-row_distinct)
    row_ranks = jnp.argsort(row_order)
    row_counts = jnp.sum((row_ranks < CAP).reshape(N_DP, RMOST).astype(jnp.int32), axis=1)
    source_cells = N_EXPERT * PEAK
    source_score = jax.random.randint(keys[3], (N_DP, N_EXPERT, PEAK), 0, 1024) + 1024 * jax.random.randint(keys[4], (N_DP, N_EXPERT, 1), 0, 16)
    forced_source = jax.random.randint(keys[5], (N_DP,), 0, N_EXPERT)
    source_score = source_score + jnp.where(jnp.arange(N_EXPERT)[None, :] == forced_source[:, None], 32768, 0)[:, :, None]
    source_distinct = source_score.reshape(N_DP, source_cells) * source_cells + jnp.arange(source_cells)[None, :]
    source_order = jnp.argsort(-source_distinct, axis=1)
    source_ranks = jnp.argsort(source_order, axis=1)
    chosen_cells = source_ranks < row_counts[:, None]
    source_counts = jnp.sum(chosen_cells.reshape(N_DP, N_EXPERT, PEAK).astype(jnp.int32), axis=2).reshape(-1)
    shuffled = jnp.argsort(jax.random.randint(keys[6], (N_DP * N_EXPERT, TOK_DEV), 0, 1073741824), axis=1)[:, :PEAK]
    candidates = jnp.arange(N_DP * N_EXPERT)[:, None] * TOK_DEV + shuffled
    usable = jnp.arange(PEAK)[None, :] < source_counts[:, None]
    sort_keys = jnp.where(usable, candidates, N_DP * N_EXPERT * TOK_DEV).reshape(-1)
    return jnp.sort(sort_keys)[:CAP].astype(jnp.int32)


def draw_selected(key, part):
    expert_keys = jax.random.split(jax.random.fold_in(key, 17), EXPERTS)
    return jax.vmap(choose_tokens)(expert_keys)


def levels(key, dims, cuts, low, largest):
    gain, own = 1.0, jax.random.fold_in(key, 6)
    for axis_at, blocks in cuts:
        draws = jnp.exp(jax.random.uniform(jax.random.fold_in(own, axis_at), (blocks,), jnp.float32, low / len(cuts), largest / len(cuts)))
        gain = gain * jnp.repeat(draws, dims[axis_at] // blocks).reshape([-1 if axis == axis_at else 1 for axis in range(len(dims))])
    return gain


def normal_values(own_key, dims, width, bound, shards=(), dtype=jnp.bfloat16):
    values = jax.random.normal(own_key, dims, jnp.float32) * width
    if len(shards) > 0:
        values = levels(own_key, dims, shards, -0.22, 0.18) * values
    return jnp.clip(values, min=-bound, max=bound).astype(dtype)


def setup_inputs(seed: int = 0) -> dict:
    seeds = jax.random.split(jax.random.key(seed), 8)
    tokens = normal_values(seeds[0], (TOKENS, D), 1.0, 6.0, ((0, 32),))
    norm_gain = jnp.clip(1.0 + 0.18 * jax.random.normal(seeds[1], (D,), jnp.float32), 0.099609375, 1.8984375).astype(jnp.bfloat16)
    router_weight = normal_values(seeds[2], (D, EXPERTS), (D // 2) ** -0.5, 0.1875)
    w_gate = normal_values(seeds[3], (EXPERTS, D, FF), D ** -0.5, 0.125, ((0, 8), (2, 4)))
    w_up = normal_values(seeds[4], (EXPERTS, D, FF), D ** -0.5, 0.125, ((0, 8), (2, 4)))
    w_down = normal_values(seeds[5], (EXPERTS, FF, D), FF ** -0.5, 0.078125, ((0, 8), (1, 4)))
    selected = draw_selected(jax.random.fold_in(seeds[7], 71), 0)
    return dict(tokens=tokens, norm_gain=norm_gain, router_weight=router_weight, w_gate=w_gate, w_up=w_up, w_down=w_down, selected=selected)


def reference(tokens, norm_gain, router_weight, w_gate, w_up, w_down, selected):
    activations = tokens.astype(jnp.float32)
    mean_square = lax.optimization_barrier(jnp.mean(activations * activations, axis=1, keepdims=True))
    normed = (activations * lax.rsqrt(mean_square + 1e-06) * norm_gain.astype(jnp.float32)).astype(jnp.bfloat16)
    gate_probs = jax.nn.sigmoid(jnp.dot(normed, router_weight, preferred_element_type=jnp.float32))
    probs_by_expert = gate_probs.T

    def per_expert(total, inputs):
        gate_matrix, up_matrix, down_matrix, chosen, probs = inputs
        expert_rows = normed[chosen]
        gate_part = jnp.dot(expert_rows, gate_matrix, preferred_element_type=jnp.float32)
        up_part = jnp.dot(expert_rows, up_matrix, preferred_element_type=jnp.float32)
        hidden = (jax.nn.gelu(gate_part, approximate=True) * up_part).astype(jnp.bfloat16)
        expert_out = jnp.dot(hidden, down_matrix, preferred_element_type=jnp.float32).astype(jnp.bfloat16)
        weights = probs[chosen]
        total = total.at[chosen].add(weights[:, None] * expert_out.astype(jnp.float32))
        return (total, None)
    start = jnp.zeros(normed.shape, jnp.float32)
    total, unused = lax.scan(per_expert, start, (w_gate, w_up, w_down, selected.astype(jnp.int32), probs_by_expert))
    return total.astype(jnp.bfloat16)
```

```python
import functools

import jax
import jax.numpy as jnp
from jax import lax
from jax.experimental import pallas as pl
from jax.experimental.pallas import tpu as pltpu
from jax.sharding import PartitionSpec as P

MESH = pl.DeviceIdType.MESH
F32 = jnp.float32
BF16 = jnp.bfloat16
CHUNKS_IN = 4
CHUNKS_OUT = 4


def tile_of(width):
    for tile in (256, 128):
        if width % tile == 0:
            return tile
    return width


def greet(experts, chips):
    me = lax.axis_index("expert")
    dp = lax.axis_index("dp")
    chip, core = dp // 2, dp % 2
    barrier = pltpu.get_barrier_semaphore()

    def expert_hello(i, carry):
        pl.semaphore_signal(
            barrier, inc=1, device_id={"expert": (me + i) % experts}, device_id_type=MESH
        )
        return carry

    lax.fori_loop(1, experts, expert_hello, 0)
    pl.semaphore_signal(
        barrier, inc=1, device_id={"dp": 2 * chip + 1 - core}, device_id_type=MESH
    )
    for i in range(1, chips):
        pl.semaphore_signal(
            barrier,
            inc=1,
            device_id={"dp": 2 * ((chip + i) % chips) + core},
            device_id_type=MESH,
        )
    pl.semaphore_wait(barrier, experts - 1 + chips)
    return me, dp, chip, core


def remote(src, dst, send_sem, recv_sem, **where):
    return pltpu.make_async_remote_copy(
        src_ref=src,
        dst_ref=dst,
        send_sem=send_sem,
        recv_sem=recv_sem,
        device_id=where,
        device_id_type=MESH,
    )


def kernel_in(
    experts, chips, chunks,
    normed, pick, pack, wg_hbm, wu_hbm, hidden,
    outgoing, received, rows, wg, wu, acc_g, acc_u,
    w_sem, a_send, a_recv, x_send, s_send, b_recv,
):
    dp_count = 2 * chips
    width = normed.shape[1] // chunks
    slots = outgoing.shape[2]
    room = rows.shape[2]
    ff = wg.shape[1]
    tile = tile_of(ff)

    def weights(k):
        part = pl.ds(k * width, width)
        return (
            pltpu.make_async_copy(wg_hbm.at[part], wg.at[part], w_sem.at[k, 0]),
            pltpu.make_async_copy(wu_hbm.at[part], wu.at[part], w_sem.at[k, 1]),
        )

    for k in range(chunks):
        for copy in weights(k):
            copy.start()
    me, dp, chip, core = greet(experts, chips)
    sibling = 2 * chip + 1 - core

    def to_expert(k, i):
        peer = (me + i) % experts
        return remote(
            outgoing.at[k, peer], received.at[k, me], a_send.at[k, peer], a_recv.at[k, me],
            expert=peer,
        )

    def from_expert(k, i):
        peer = (me + i) % experts
        return remote(
            outgoing.at[k, peer], received.at[k, peer], a_send.at[k, peer], a_recv.at[k, peer],
            expert=peer,
        )

    def to_chip(k, i):
        other = 2 * ((chip + i) % chips) + core
        return remote(
            rows.at[k, dp], rows.at[k, dp], x_send.at[k, i], b_recv.at[k, dp], dp=other
        )

    def from_chip(k, i):
        other = 2 * ((chip + i) % chips) + core
        return remote(
            rows.at[k, other], rows.at[k, other], x_send.at[k, i], b_recv.at[k, other], dp=other
        )

    def to_sibling(k, i):
        block = 2 * ((chip + i) % chips) + core
        return remote(
            rows.at[k, block], rows.at[k, block], s_send.at[k, i], b_recv.at[k, block],
            dp=sibling,
        )

    def from_sibling(k, i):
        block = 2 * ((chip + i) % chips) + 1 - core
        return remote(
            rows.at[k, block], rows.at[k, block], s_send.at[k, i], b_recv.at[k, block],
            dp=sibling,
        )

    for k in range(chunks):
        chosen = jnp.dot(
            pick[...], normed[:, k * width : (k + 1) * width], preferred_element_type=F32
        )
        outgoing[k] = chosen.astype(BF16).reshape(experts, slots, width)

        def send(i, carry):
            to_expert(k, i).start()
            return carry

        lax.fori_loop(1, experts, send, 0)
        received[k, me] = outgoing[k, me]

    for step in range(chunks + 2):
        if step < chunks:

            def take(i, carry):
                from_expert(step, i).wait_recv()
                return carry

            lax.fori_loop(1, experts, take, 0)
            packed = jnp.dot(
                pack[...],
                received[step].reshape(experts * slots, width),
                preferred_element_type=F32,
            )
            rows[step, dp] = packed.astype(BF16)
            for i in range(1, chips):
                to_chip(step, i).start()
            to_sibling(step, 0).start()
        if 1 <= step <= chunks:
            for i in range(1, chips):
                from_chip(step - 1, i).wait_recv()
                to_sibling(step - 1, i).start()
        if step >= 2:
            k = step - 2
            for i in range(chips):
                from_sibling(k, i).wait_recv()
            for copy in weights(k):
                copy.wait()

            def multiply(n, carry):
                cols = pl.ds(pl.multiple_of(n * tile, tile), tile)
                depth = pl.ds(k * width, width)
                block = rows[k].reshape(dp_count * room, width)
                g = jnp.dot(block, wg[depth, cols], preferred_element_type=F32)
                u = jnp.dot(block, wu[depth, cols], preferred_element_type=F32)
                if k > 0:
                    g = g + acc_g[:, cols]
                    u = u + acc_u[:, cols]
                if k < chunks - 1:
                    acc_g[:, cols] = g
                    acc_u[:, cols] = u
                else:
                    hidden[:, cols] = (jax.nn.gelu(g, approximate=True) * u).astype(BF16)
                return carry

            lax.fori_loop(0, ff // tile, multiply, 0)

    for k in range(chunks):

        def sent(i, carry):
            to_expert(k, i).wait_send()
            return carry

        lax.fori_loop(1, experts, sent, 0)
        for i in range(1, chips):
            to_chip(k, i).wait_send()
        for i in range(chips):
            to_sibling(k, i).wait_send()


def kernel_out(
    experts, chips, chunks,
    hidden, unpack, mixing, wd_hbm, out,
    wd, own, sib_out, sib_in, x_out, x_in, returning, arrived, mix_high, mix_low,
    w_sem, s_send, s_recv, x_send, x_recv, a_send, a_recv,
):
    width = out.shape[1] // chunks
    slots = arrived.shape[2]

    def weights(k):
        part = pl.ds(k * width, width)
        return pltpu.make_async_copy(wd_hbm.at[:, part], wd.at[k], w_sem.at[k])

    for k in range(chunks):
        weights(k).start()
    me, dp, chip, core = greet(experts, chips)
    sibling = 2 * chip + 1 - core
    high = mixing[...].astype(BF16)
    mix_high[...] = high
    mix_low[...] = (mixing[...] - high.astype(F32)).astype(BF16)

    def sib_copy(k, i):
        return remote(
            sib_out.at[k, i], sib_in.at[k, i], s_send.at[k, i], s_recv.at[k, i], dp=sibling
        )

    def chip_copy(k, i):
        return remote(
            x_out.at[k, i - 1], x_in.at[k, i - 1], x_send.at[k, i - 1], x_recv.at[k, i - 1],
            dp=2 * ((chip + i) % chips) + core,
        )

    def to_expert(k, i):
        peer = (me + i) % experts
        return remote(
            returning.at[k, peer], arrived.at[k, me], a_send.at[k, peer], a_recv.at[k, me],
            expert=peer,
        )

    def from_expert(k, i):
        peer = (me + i) % experts
        return remote(
            returning.at[k, peer], arrived.at[k, peer], a_send.at[k, peer], a_recv.at[k, peer],
            expert=peer,
        )

    for step in range(chunks + 3):
        if step < chunks:
            k = step
            weights(k).wait()

            def give(i, carry):
                block = 2 * ((chip + i) % chips) + 1 - core
                term = jnp.dot(hidden[block], wd[k], preferred_element_type=F32)
                sib_out[k, i] = term.astype(BF16)
                sib_copy(k, i).start()
                return carry

            lax.fori_loop(0, chips, give, 0)

            def keep(i, carry):
                block = 2 * ((chip + i) % chips) + core
                own[k, i] = jnp.dot(hidden[block], wd[k], preferred_element_type=F32)
                return carry

            lax.fori_loop(0, chips, keep, 0)
        if 1 <= step <= chunks:
            k = step - 1
            for i in range(chips):
                sib_copy(k, i).wait_recv()
            for i in range(1, chips):
                x_out[k, i - 1] = (own[k, i] + sib_in[k, i].astype(F32)).astype(BF16)
                chip_copy(k, i).start()
        if 2 <= step <= chunks + 1:
            k = step - 2
            total = own[k, 0] + sib_in[k, 0].astype(F32)
            for i in range(1, chips):
                chip_copy(k, i).wait_recv()
                total = total + x_in[k, i - 1].astype(F32)
            spread = jnp.dot(unpack[...], total.astype(BF16), preferred_element_type=F32)
            returning[k] = spread.astype(BF16).reshape(experts, slots, width)

            def send(i, carry):
                to_expert(k, i).start()
                return carry

            lax.fori_loop(1, experts, send, 0)
            arrived[k, me] = returning[k, me]
        if step >= 3:
            k = step - 3

            def take(i, carry):
                from_expert(k, i).wait_recv()
                return carry

            lax.fori_loop(1, experts, take, 0)
            values = arrived[k].reshape(experts * slots, width)
            combined = jnp.dot(mix_high[...], values, preferred_element_type=F32)
            combined = combined + jnp.dot(mix_low[...], values, preferred_element_type=F32)
            out[:, k * width : (k + 1) * width] = combined.astype(BF16)

    for k in range(chunks):
        for i in range(chips):
            sib_copy(k, i).wait_send()
        for i in range(1, chips):
            chip_copy(k, i).wait_send()

        def sent(i, carry):
            to_expert(k, i).wait_send()
            return carry

        lax.fori_loop(1, experts, sent, 0)


def per_device(tokens, norm_gain, router_weight, w_gate, w_up, w_down, selected):
    dp_count = lax.axis_size("dp")
    experts = lax.axis_size("expert")
    chips = dp_count // 2
    tok_rows, model_width = tokens.shape
    capacity = selected.shape[1]
    ff = w_gate.shape[2]
    slots = 4 * tok_rows // experts
    room = 3 * capacity // (2 * dp_count)
    dp_index = lax.axis_index("dp")
    expert_index = lax.axis_index("expert")
    source = dp_index * experts + expert_index
    activations = tokens.astype(F32)
    mean_square = jnp.mean(activations * activations, axis=1, keepdims=True)
    normed = (activations * lax.rsqrt(mean_square + 1e-06) * norm_gain.astype(F32)).astype(BF16)
    gate_probs = jax.nn.sigmoid(jnp.dot(normed, router_weight, preferred_element_type=F32))

    mine = source * tok_rows + jnp.arange(tok_rows, dtype=jnp.int32)
    member = jnp.any(selected[:, :, None] == mine[None, None, :], axis=1)
    order = jnp.arange(tok_rows, dtype=jnp.int32)
    before = (order[:, None] < order[None, :]).astype(BF16)
    rank = jnp.dot(member.astype(BF16), before, preferred_element_type=F32)
    slot = jnp.arange(slots, dtype=F32)
    chosen = member[:, None, :] & (rank[:, None, :] == slot[None, :, None])
    pick = chosen.astype(BF16).reshape(experts * slots, tok_rows)
    mixing = jnp.where(chosen, gate_probs.T[:, None, :], 0.0).reshape(experts * slots, tok_rows).T

    expert_row = lax.dynamic_index_in_dim(selected, expert_index, 0, keepdims=False)
    senders = jnp.arange(experts, dtype=jnp.int32)
    first_token = (dp_index * experts + senders) * tok_rows
    firsts = jnp.sum((expert_row[None, :] < first_token[:, None]).astype(jnp.int32), axis=1)
    lasts = jnp.sum(
        (expert_row[None, :] < first_token[:, None] + tok_rows).astype(jnp.int32), axis=1
    )
    places = jnp.arange(slots, dtype=jnp.int32)
    target = jnp.where(
        places[None, :] < (lasts - firsts)[:, None],
        (firsts - firsts[0])[:, None] + places[None, :],
        -1,
    ).reshape(-1)
    spots = jnp.arange(room, dtype=jnp.int32)
    pack = (spots[:, None] == target[None, :]).astype(BF16)
    unpack = (target[:, None] == spots[None, :]).astype(BF16)

    in_vmem = pl.BlockSpec(memory_space=pltpu.VMEM)
    in_any = pl.BlockSpec(memory_space=pl.ANY)
    dma = pltpu.SemaphoreType.DMA
    all_rows = dp_count * room
    chunks = CHUNKS_IN
    width = model_width // chunks
    hidden = pl.pallas_call(
        functools.partial(kernel_in, experts, chips, chunks),
        out_shape=jax.ShapeDtypeStruct((all_rows, ff), BF16),
        in_specs=[in_vmem, in_vmem, in_vmem, in_any, in_any],
        out_specs=in_vmem,
        scratch_shapes=[
            pltpu.VMEM((chunks, experts, slots, width), BF16),
            pltpu.VMEM((chunks, experts, slots, width), BF16),
            pltpu.VMEM((chunks, dp_count, room, width), BF16),
            pltpu.VMEM((model_width, ff), BF16),
            pltpu.VMEM((model_width, ff), BF16),
            pltpu.VMEM((all_rows, ff), F32),
            pltpu.VMEM((all_rows, ff), F32),
            dma((chunks, 2)),
            dma((chunks, experts)),
            dma((chunks, experts)),
            dma((chunks, chips)),
            dma((chunks, chips)),
            dma((chunks, dp_count)),
        ],
        compiler_params=pltpu.CompilerParams(
            collective_id=0, has_side_effects=True, vmem_limit_bytes=60 * 2**20
        ),
        name="dispatch",
    )(normed, pick, pack, w_gate[0], w_up[0])

    chunks = CHUNKS_OUT
    width = model_width // chunks
    return pl.pallas_call(
        functools.partial(kernel_out, experts, chips, chunks),
        out_shape=jax.ShapeDtypeStruct((tok_rows, model_width), BF16),
        in_specs=[in_vmem, in_vmem, in_vmem, in_any],
        out_specs=in_vmem,
        scratch_shapes=[
            pltpu.VMEM((chunks, ff, width), BF16),
            pltpu.VMEM((chunks, chips, room, width), F32),
            pltpu.VMEM((chunks, chips, room, width), BF16),
            pltpu.VMEM((chunks, chips, room, width), BF16),
            pltpu.VMEM((chunks, max(chips - 1, 1), room, width), BF16),
            pltpu.VMEM((chunks, max(chips - 1, 1), room, width), BF16),
            pltpu.VMEM((chunks, experts, slots, width), BF16),
            pltpu.VMEM((chunks, experts, slots, width), BF16),
            pltpu.VMEM((tok_rows, experts * slots), BF16),
            pltpu.VMEM((tok_rows, experts * slots), BF16),
            dma((chunks,)),
            dma((chunks, chips)),
            dma((chunks, chips)),
            dma((chunks, max(chips - 1, 1))),
            dma((chunks, max(chips - 1, 1))),
            dma((chunks, experts)),
            dma((chunks, experts)),
        ],
        compiler_params=pltpu.CompilerParams(
            collective_id=1, has_side_effects=True, vmem_limit_bytes=60 * 2**20
        ),
        name="combine",
    )(hidden.reshape(dp_count, room, ff), unpack, mixing, w_down[0])


def solution(mesh):
    in_specs = (
        P(("dp", "expert"), None),
        P(),
        P(),
        P("expert", None, "dp"),
        P("expert", None, "dp"),
        P("expert", "dp", None),
        P(),
    )
    out_specs = P(("dp", "expert"), None)
    return jax.shard_map(
        per_device, mesh=mesh, in_specs=in_specs, out_specs=out_specs, check_vma=False
    )
```

```python
import functools

import jax
import jax.numpy as jnp
from jax import lax
from jax.experimental import pallas as pl
from jax.experimental.pallas import tpu as pltpu
from jax.sharding import PartitionSpec as P

MESH = pl.DeviceIdType.MESH
F32 = jnp.float32
BF16 = jnp.bfloat16
CHUNKS_IN = 8
CHUNKS_OUT = 8
AHEAD = 2


def tile_of(width):
    for tile in (256, 128):
        if width % tile == 0:
            return tile
    return width


def greet(experts, chips):
    me = lax.axis_index("expert")
    dp = lax.axis_index("dp")
    chip, core = dp // 2, dp % 2
    barrier = pltpu.get_barrier_semaphore()

    half = experts // 2
    base, local = (me // half) * half, me % half

    def expert_hello(i, carry):
        pl.semaphore_signal(
            barrier, inc=1, device_id={"expert": base + (local + i) % half}, device_id_type=MESH
        )
        return carry

    lax.fori_loop(1, half, expert_hello, 0)
    pl.semaphore_signal(
        barrier, inc=1, device_id={"expert": (me + half) % experts}, device_id_type=MESH
    )
    pl.semaphore_signal(
        barrier, inc=1, device_id={"dp": 2 * chip + 1 - core}, device_id_type=MESH
    )
    for i in range(1, chips):
        pl.semaphore_signal(
            barrier,
            inc=1,
            device_id={"dp": 2 * ((chip + i) % chips) + core},
            device_id_type=MESH,
        )
    pl.semaphore_wait(barrier, half + chips)
    return me, dp, chip, core


def remote(src, dst, send_sem, recv_sem, **where):
    return pltpu.make_async_remote_copy(
        src_ref=src,
        dst_ref=dst,
        send_sem=send_sem,
        recv_sem=recv_sem,
        device_id=where,
        device_id_type=MESH,
    )


def kernel_in(
    experts, chips, chunks,
    normed, pick, pack, wg_hbm, wu_hbm, hidden,
    tok_out, tok_in, outgoing, received, rows, wg, wu, acc_g, acc_u,
    w_sem, t_send, t_recv, a_send, a_recv, x_send, s_send, b_recv,
):
    half = experts // 2
    dp_count = 2 * chips
    width = normed.shape[1] // chunks
    slots = received.shape[2]
    room = rows.shape[2]
    ff = wg.shape[1]
    tile = tile_of(ff)

    def weights(k):
        part = pl.ds(k * width, width)
        return (
            pltpu.make_async_copy(wg_hbm.at[part], wg.at[part], w_sem.at[k, 0]),
            pltpu.make_async_copy(wu_hbm.at[part], wu.at[part], w_sem.at[k, 1]),
        )

    for k in range(chunks):
        tok_out[k] = normed[:, k * width : (k + 1) * width]
    me, dp, chip, core = greet(experts, chips)
    base, local = (me // half) * half, me % half
    partner = (me + half) % experts
    sibling = 2 * chip + 1 - core

    def to_partner(k):
        return remote(
            tok_out.at[k], tok_in.at[k], t_send.at[k], t_recv.at[k], expert=partner
        )

    def to_expert(k, side, i):
        near = (local + i) % half
        owner = (me + side * half) % experts
        return remote(
            outgoing.at[k, side, near], received.at[k, owner],
            a_send.at[k, side, near], a_recv.at[k, owner], expert=base + near,
        )

    def from_expert(k, side, i):
        near = (local + i) % half
        owner = (base + near + side * half) % experts
        return remote(
            outgoing.at[k, side, near], received.at[k, owner],
            a_send.at[k, side, near], a_recv.at[k, owner], expert=base + near,
        )

    def to_chip(k, i):
        other = 2 * ((chip + i) % chips) + core
        return remote(
            rows.at[k, dp], rows.at[k, dp], x_send.at[k, i], b_recv.at[k, dp], dp=other
        )

    def from_chip(k, i):
        other = 2 * ((chip + i) % chips) + core
        return remote(
            rows.at[k, other], rows.at[k, other], x_send.at[k, i], b_recv.at[k, other], dp=other
        )

    def to_sibling(k, i):
        block = 2 * ((chip + i) % chips) + core
        return remote(
            rows.at[k, block], rows.at[k, block], s_send.at[k, i], b_recv.at[k, block],
            dp=sibling,
        )

    def from_sibling(k, i):
        block = 2 * ((chip + i) % chips) + 1 - core
        return remote(
            rows.at[k, block], rows.at[k, block], s_send.at[k, i], b_recv.at[k, block],
            dp=sibling,
        )

    def send_rows(k, side, source):
        chosen = jnp.dot(pick[side], source, preferred_element_type=F32)
        outgoing[k, side] = chosen.astype(BF16).reshape(half, slots, width)

        def send(i, carry):
            to_expert(k, side, i).start()
            return carry

        lax.fori_loop(1, half, send, 0)
        received[k, (me + side * half) % experts] = outgoing[k, side, local]

    for k in range(min(AHEAD, chunks)):
        to_partner(k).start()
    send_rows(0, 0, tok_out[0])
    for k in range(chunks):
        for copy in weights(k):
            copy.start()

    for step in range(chunks + 3):
        if step + AHEAD < chunks:
            to_partner(step + AHEAD).start()
        if step + 1 < chunks:
            send_rows(step + 1, 0, tok_out[step + 1])
        if step < chunks:
            to_partner(step).wait_recv()
            send_rows(step, 1, tok_in[step])
        if 1 <= step <= chunks:
            k = step - 1

            def take(i, carry):
                from_expert(k, 0, i).wait_recv()
                from_expert(k, 1, i).wait_recv()
                return carry

            lax.fori_loop(1, half, take, 0)
            packed = jnp.dot(
                pack[...],
                received[k].reshape(experts * slots, width),
                preferred_element_type=F32,
            )
            rows[k, dp] = packed.astype(BF16)
            for i in range(1, chips):
                to_chip(k, i).start()
            to_sibling(k, 0).start()
        if 2 <= step <= chunks + 1:
            for i in range(1, chips):
                from_chip(step - 2, i).wait_recv()
                to_sibling(step - 2, i).start()
        if step >= 3:
            k = step - 3
            for i in range(chips):
                from_sibling(k, i).wait_recv()
            for copy in weights(k):
                copy.wait()

            def multiply(n, carry):
                cols = pl.ds(pl.multiple_of(n * tile, tile), tile)
                depth = pl.ds(k * width, width)
                block = rows[k].reshape(dp_count * room, width)
                g = jnp.dot(block, wg[depth, cols], preferred_element_type=F32)
                u = jnp.dot(block, wu[depth, cols], preferred_element_type=F32)
                if k > 0:
                    g = g + acc_g[:, cols]
                    u = u + acc_u[:, cols]
                if k < chunks - 1:
                    acc_g[:, cols] = g
                    acc_u[:, cols] = u
                else:
                    hidden[:, cols] = (jax.nn.gelu(g, approximate=True) * u).astype(BF16)
                return carry

            lax.fori_loop(0, ff // tile, multiply, 0)

    for k in range(chunks):
        to_partner(k).wait_send()

        def sent(i, carry):
            to_expert(k, 0, i).wait_send()
            to_expert(k, 1, i).wait_send()
            return carry

        lax.fori_loop(1, half, sent, 0)
        for i in range(1, chips):
            to_chip(k, i).wait_send()
        for i in range(chips):
            to_sibling(k, i).wait_send()


def kernel_out(
    experts, chips, chunks,
    hidden, unpack, mixing, wd_hbm, out,
    wd, own, sib_out, sib_in, x_out, x_in, returning, arrived, tok_out, tok_in,
    mix_high, mix_low,
    w_sem, s_send, s_recv, x_send, x_recv, a_send, a_recv, t_send, t_recv,
):
    half = experts // 2
    width = out.shape[1] // chunks
    slots = arrived.shape[3]

    def weights(k):
        part = pl.ds(k * width, width)
        return pltpu.make_async_copy(wd_hbm.at[:, part], wd.at[k], w_sem.at[k])

    for k in range(chunks):
        weights(k).start()
    me, dp, chip, core = greet(experts, chips)
    base, local = (me // half) * half, me % half
    partner = (me + half) % experts
    sibling = 2 * chip + 1 - core
    high = mixing[...].astype(BF16)
    mix_high[...] = high
    mix_low[...] = (mixing[...] - high.astype(F32)).astype(BF16)

    def sib_copy(k, i):
        return remote(
            sib_out.at[k, i], sib_in.at[k, i], s_send.at[k, i], s_recv.at[k, i], dp=sibling
        )

    def chip_copy(k, i):
        return remote(
            x_out.at[k, i - 1], x_in.at[k, i - 1], x_send.at[k, i - 1], x_recv.at[k, i - 1],
            dp=2 * ((chip + i) % chips) + core,
        )

    def to_expert(k, side, i):
        near = (local + i) % half
        owner = (base + near + side * half) % experts
        return remote(
            returning.at[k, owner], arrived.at[k, side, local],
            a_send.at[k, owner], a_recv.at[k, side, local], expert=base + near,
        )

    def from_expert(k, side, i):
        near = (local + i) % half
        owner = (base + near + side * half) % experts
        return remote(
            returning.at[k, owner], arrived.at[k, side, near],
            a_send.at[k, owner], a_recv.at[k, side, near], expert=base + near,
        )

    def to_partner(k):
        return remote(
            tok_out.at[k], tok_in.at[k], t_send.at[k], t_recv.at[k], expert=partner
        )

    def mixed(k, side):
        values = arrived[k, side].reshape(half * slots, width)
        sums = jnp.dot(mix_high[side], values, preferred_element_type=F32)
        return sums + jnp.dot(mix_low[side], values, preferred_element_type=F32)

    def take_side(k, side):
        def take(i, carry):
            from_expert(k, side, i).wait_recv()
            return carry

        lax.fori_loop(1, half, take, 0)

    for step in range(chunks + 4):
        if step < chunks:
            k = step
            weights(k).wait()

            def give(i, carry):
                block = 2 * ((chip + i) % chips) + 1 - core
                term = jnp.dot(hidden[block], wd[k], preferred_element_type=F32)
                sib_out[k, i] = term.astype(BF16)
                sib_copy(k, i).start()
                return carry

            lax.fori_loop(0, chips, give, 0)

            def keep(i, carry):
                block = 2 * ((chip + i) % chips) + core
                own[k, i] = jnp.dot(hidden[block], wd[k], preferred_element_type=F32)
                return carry

            lax.fori_loop(0, chips, keep, 0)
        if 1 <= step <= chunks:
            k = step - 1
            for i in range(chips):
                sib_copy(k, i).wait_recv()
            for i in range(1, chips):
                x_out[k, i - 1] = (own[k, i] + sib_in[k, i].astype(F32)).astype(BF16)
                chip_copy(k, i).start()
        if 2 <= step <= chunks + 1:
            k = step - 2
            total = own[k, 0] + sib_in[k, 0].astype(F32)
            for i in range(1, chips):
                chip_copy(k, i).wait_recv()
                total = total + x_in[k, i - 1].astype(F32)
            spread = jnp.dot(unpack[...], total.astype(BF16), preferred_element_type=F32)
            returning[k] = spread.astype(BF16).reshape(experts, slots, width)
            for side in (1, 0):

                def send(i, carry):
                    to_expert(k, side, i).start()
                    return carry

                lax.fori_loop(1, half, send, 0)
                arrived[k, side, local] = returning[k, (me + side * half) % experts]
        if 3 <= step <= chunks + 2:
            k = step - 3
            take_side(k, 1)
            tok_out[k] = mixed(k, 1).astype(BF16)
            to_partner(k).start()
        if step >= 4:
            k = step - 4
            take_side(k, 0)
            near_sum = mixed(k, 0)
            to_partner(k).wait_recv()
            combined = near_sum + tok_in[k].astype(F32)
            out[:, k * width : (k + 1) * width] = combined.astype(BF16)

    for k in range(chunks):
        for i in range(chips):
            sib_copy(k, i).wait_send()
        for i in range(1, chips):
            chip_copy(k, i).wait_send()
        to_partner(k).wait_send()

        def sent(i, carry):
            to_expert(k, 0, i).wait_send()
            to_expert(k, 1, i).wait_send()
            return carry

        lax.fori_loop(1, half, sent, 0)


def per_device(tokens, norm_gain, router_weight, w_gate, w_up, w_down, selected):
    dp_count = lax.axis_size("dp")
    experts = lax.axis_size("expert")
    chips = dp_count // 2
    tok_rows, model_width = tokens.shape
    capacity = selected.shape[1]
    ff = w_gate.shape[2]
    slots = 4 * tok_rows // experts
    room = 3 * capacity // (2 * dp_count)
    dp_index = lax.axis_index("dp")
    expert_index = lax.axis_index("expert")
    activations = tokens.astype(F32)
    mean_square = jnp.mean(activations * activations, axis=1, keepdims=True)
    normed = (activations * lax.rsqrt(mean_square + 1e-06) * norm_gain.astype(F32)).astype(BF16)
    gate_probs = jax.nn.sigmoid(jnp.dot(normed, router_weight, preferred_element_type=F32))

    half = experts // 2
    base = (expert_index // half) * half
    partner = (expert_index + half) % experts
    near = lax.dynamic_slice_in_dim(selected, base, half, 0)
    pair = dp_index * experts + jnp.stack([expert_index, partner])
    order = jnp.arange(tok_rows, dtype=jnp.int32)
    ours = (pair[:, None] * tok_rows + order[None, :]).reshape(-1)
    member = jnp.any(near[:, :, None] == ours[None, None, :], axis=1)
    member = member.reshape(half * 2, tok_rows)
    before = (order[:, None] < order[None, :]).astype(BF16)
    rank = jnp.dot(member.astype(BF16), before, preferred_element_type=F32)
    slot = jnp.arange(slots, dtype=F32)
    place = jnp.where(member, rank, -1.0).reshape(half, 2, tok_rows).transpose(1, 0, 2)
    chosen = place[:, :, None, :] == slot[None, None, :, None]
    pick = chosen.astype(BF16).reshape(2, half * slots, tok_rows)
    swap = [(e, (e + half) % experts) for e in range(experts)]
    far_probs = lax.ppermute(gate_probs, "expert", swap)
    probs = lax.dynamic_slice_in_dim(jnp.stack([gate_probs, far_probs]), base, half, 2)
    placed = place.transpose(0, 2, 1)
    mixing = jnp.where(
        placed[:, :, :, None] == slot[None, None, None, :], probs[:, :, :, None], 0.0
    ).reshape(2, tok_rows, half * slots)

    expert_row = lax.dynamic_index_in_dim(selected, expert_index, 0, keepdims=False)
    senders = jnp.arange(experts, dtype=jnp.int32)
    first_token = (dp_index * experts + senders) * tok_rows
    firsts = jnp.sum((expert_row[None, :] < first_token[:, None]).astype(jnp.int32), axis=1)
    lasts = jnp.sum(
        (expert_row[None, :] < first_token[:, None] + tok_rows).astype(jnp.int32), axis=1
    )
    places = jnp.arange(slots, dtype=jnp.int32)
    target = jnp.where(
        places[None, :] < (lasts - firsts)[:, None],
        (firsts - firsts[0])[:, None] + places[None, :],
        -1,
    ).reshape(-1)
    spots = jnp.arange(room, dtype=jnp.int32)
    pack = (spots[:, None] == target[None, :]).astype(BF16)
    unpack = (target[:, None] == spots[None, :]).astype(BF16)

    in_vmem = pl.BlockSpec(memory_space=pltpu.VMEM)
    in_any = pl.BlockSpec(memory_space=pl.ANY)
    dma = pltpu.SemaphoreType.DMA
    all_rows = dp_count * room
    chunks = CHUNKS_IN
    width = model_width // chunks
    hidden = pl.pallas_call(
        functools.partial(kernel_in, experts, chips, chunks),
        out_shape=jax.ShapeDtypeStruct((all_rows, ff), BF16),
        in_specs=[in_vmem, in_vmem, in_vmem, in_any, in_any],
        out_specs=in_vmem,
        scratch_shapes=[
            pltpu.VMEM((chunks, tok_rows, width), BF16),
            pltpu.VMEM((chunks, tok_rows, width), BF16),
            pltpu.VMEM((chunks, 2, half, slots, width), BF16),
            pltpu.VMEM((chunks, experts, slots, width), BF16),
            pltpu.VMEM((chunks, dp_count, room, width), BF16),
            pltpu.VMEM((model_width, ff), BF16),
            pltpu.VMEM((model_width, ff), BF16),
            pltpu.VMEM((all_rows, ff), F32),
            pltpu.VMEM((all_rows, ff), F32),
            dma((chunks, 2)),
            dma((chunks,)),
            dma((chunks,)),
            dma((chunks, 2, half)),
            dma((chunks, experts)),
            dma((chunks, chips)),
            dma((chunks, chips)),
            dma((chunks, dp_count)),
        ],
        compiler_params=pltpu.CompilerParams(
            collective_id=0, has_side_effects=True, vmem_limit_bytes=60 * 2**20
        ),
        name="dispatch",
    )(normed, pick, pack, w_gate[0], w_up[0])

    chunks = CHUNKS_OUT
    width = model_width // chunks
    return pl.pallas_call(
        functools.partial(kernel_out, experts, chips, chunks),
        out_shape=jax.ShapeDtypeStruct((tok_rows, model_width), BF16),
        in_specs=[in_vmem, in_vmem, in_vmem, in_any],
        out_specs=in_vmem,
        scratch_shapes=[
            pltpu.VMEM((chunks, ff, width), BF16),
            pltpu.VMEM((chunks, chips, room, width), F32),
            pltpu.VMEM((chunks, chips, room, width), BF16),
            pltpu.VMEM((chunks, chips, room, width), BF16),
            pltpu.VMEM((chunks, max(chips - 1, 1), room, width), BF16),
            pltpu.VMEM((chunks, max(chips - 1, 1), room, width), BF16),
            pltpu.VMEM((chunks, experts, slots, width), BF16),
            pltpu.VMEM((chunks, 2, half, slots, width), BF16),
            pltpu.VMEM((chunks, tok_rows, width), BF16),
            pltpu.VMEM((chunks, tok_rows, width), BF16),
            pltpu.VMEM((2, tok_rows, half * slots), BF16),
            pltpu.VMEM((2, tok_rows, half * slots), BF16),
            dma((chunks,)),
            dma((chunks, chips)),
            dma((chunks, chips)),
            dma((chunks, max(chips - 1, 1))),
            dma((chunks, max(chips - 1, 1))),
            dma((chunks, experts)),
            dma((chunks, 2, half)),
            dma((chunks,)),
            dma((chunks,)),
        ],
        compiler_params=pltpu.CompilerParams(
            collective_id=1, has_side_effects=True, vmem_limit_bytes=60 * 2**20
        ),
        name="combine",
    )(hidden.reshape(dp_count, room, ff), unpack, mixing, w_down[0])


def solution(mesh):
    in_specs = (
        P(("dp", "expert"), None),
        P(),
        P(),
        P("expert", None, "dp"),
        P("expert", None, "dp"),
        P("expert", "dp", None),
        P(),
    )
    out_specs = P(("dp", "expert"), None)
    return jax.shard_map(
        per_device, mesh=mesh, in_specs=in_specs, out_specs=out_specs, check_vma=False
    )
```
